32 devices in a mesh: gx: 4 (over x, core), gy: 4 (over z), gz: 2 (over y).
Axes of the slice: x: 2, y: 2, z: 4, core: 2. Of those that a mesh axis runs over, the one named last changes fastest.
Arguments:
- relative_placements: float32 [3, 12, 12, 8, 128], P(None, 'gx', 'gy', 'gz'), may hold values from 0 to 1
- mass_per_density: float32 [12, 12, 8, 128], P('gx', 'gy', 'gz'), may hold values from 0.004 to 0.04
- opening_heat_level: float32 [12, 12, 8, 128], P('gx', 'gy', 'gz'), may hold values from 0.5 to 2
- bin_fill_counts: int32 [12, 12, 8], P('gx', 'gy', 'gz'), may hold values from 16 to 128
Outputs:
- final_temp: float32 [12, 12, 8, 128], P('gx', 'gy', 'gz')
The draws below stay inside these ranges and needn't reach their ends.
Inputs may be any that keep to these rules, and one draw needn't show every extreme that they name: Tile cell t holds particles in slots 0 to bin_fill_counts[t] - 1; the other slots are empty and are no source.
All inputs are finite; a program needn't handle non-finite values.
Results may differ from the reference program's by a relative error of at most 0.0003.
Values sent between devices are 32-bit elements; how exact they have to be, the bound alone decides.
A program may use at most 64 MiB of HBM per device.

```python
import math
import jax
import jax.numpy as jnp
from jax import lax

BIN_CAPACITY = 128
BLOCK_SPAN_EAST = 12
BLOCK_SPAN_NORTH = 12
BLOCK_SPAN_UPWARD = 8


def with_ends(drawn, own_key, least, largest):
    shape = drawn.shape
    spot = [jax.random.randint(jax.random.fold_in(own_key, axis), (), 0, shape[axis]) for axis in range(len(shape))]
    drawn = drawn.at[tuple(spot)].set(least)
    longest = shape.index(max(shape))
    spot[longest] = (spot[longest] + 1) % shape[longest]
    return drawn.at[tuple(spot)].set(largest)


def levels(rng, extent, split, least, largest):
    factor_of = 1.0
    for dim, shards_of in split:
        draws = jax.random.uniform(jax.random.fold_in(jax.random.fold_in(rng, 6), dim), (shards_of,), jnp.float32, least / len(split), largest / len(split))
        factor_of = factor_of * jnp.repeat(jnp.exp(draws), extent[dim] // shards_of).reshape((-1,) + (1,) * (len(extent) - 1 - dim))
    return factor_of


def setup_inputs(seed: int = 0) -> dict:
    keys = jax.random.split(jax.random.key(seed), 5)
    return {
        "relative_placements": jnp.clip(1.0 * jax.random.uniform(keys[0], (3, BLOCK_SPAN_EAST, BLOCK_SPAN_NORTH, BLOCK_SPAN_UPWARD, BIN_CAPACITY), jnp.float32) ** levels(keys[0], (3, BLOCK_SPAN_EAST, BLOCK_SPAN_NORTH, BLOCK_SPAN_UPWARD, BIN_CAPACITY), ((1, 4), (2, 4), (3, 2)), -0.2, 0.2), 0.0, 1.0),
        "mass_per_density": jnp.clip(jnp.exp(math.log(0.04) - 2.30258502 * jax.random.uniform(keys[1], (BLOCK_SPAN_EAST, BLOCK_SPAN_NORTH, BLOCK_SPAN_UPWARD, BIN_CAPACITY), jnp.float32) ** levels(keys[1], (BLOCK_SPAN_EAST, BLOCK_SPAN_NORTH, BLOCK_SPAN_UPWARD, BIN_CAPACITY), ((0, 4), (1, 4), (2, 2)), -0.2, 0.2)), 0.004, 0.04),
        "opening_heat_level": jnp.clip(jnp.exp(math.log(2.0) - 1.3862944 * jax.random.uniform(keys[2], (BLOCK_SPAN_EAST, BLOCK_SPAN_NORTH, BLOCK_SPAN_UPWARD, BIN_CAPACITY), jnp.float32) ** levels(keys[2], (BLOCK_SPAN_EAST, BLOCK_SPAN_NORTH, BLOCK_SPAN_UPWARD, BIN_CAPACITY), ((0, 4), (1, 4), (2, 2)), -0.2, 0.2)), 0.5, 2.0),
        "bin_fill_counts": with_ends(jax.random.randint(keys[3], (BLOCK_SPAN_EAST, BLOCK_SPAN_NORTH, BLOCK_SPAN_UPWARD), BIN_CAPACITY // 8, BIN_CAPACITY + 1), jax.random.fold_in(keys[3], 1), BIN_CAPACITY // 8, BIN_CAPACITY).astype(jnp.int32),
    }


step_factor = 2.0

def conduct(fields, periodic_enclosure):
    extent_x, extent_y, extent_z = periodic_enclosure
    bin_dimensions = fields.shape[-1]

    def one_column(column):
        col_x = column // extent_y
        col_y = column % extent_y

        def column_at(shift_x, shift_y):
            column_part = lax.dynamic_slice_in_dim(fields, col_x + 1 + shift_x, 1, 1)
            column_part = lax.dynamic_slice_in_dim(column_part, col_y + 1 + shift_y, 1, 2)
            return column_part[:, 0, 0]
        target = column_at(0, 0)[:, 1:1 + extent_z]
        inflow = jnp.zeros((extent_z, bin_dimensions), jnp.float32)
        weights = jnp.zeros((extent_z, bin_dimensions), jnp.float32)
        for shift_x in (-1, 0, 1):
            for shift_y in (-1, 0, 1):
                source_col = column_at(shift_x, shift_y)
                for shift_z in (-1, 0, 1):
                    source = source_col[:, 1 + shift_z:1 + shift_z + extent_z]
                    dist_sq = (float(shift_x) + source[0][:, None, :] - target[0][:, :, None]) ** 2
                    dist_sq = dist_sq + (float(shift_y) + source[1][:, None, :] - target[1][:, :, None]) ** 2
                    dist_sq = dist_sq + (float(shift_z) + source[2][:, None, :] - target[2][:, :, None]) ** 2
                    kernel = jnp.maximum(1.0 - jnp.sqrt(dist_sq), 0.0) ** 3
                    pair = kernel * source[3][:, None, :] * (target[5][:, :, None] + source[5][:, None, :])
                    inflow = inflow + lax.optimization_barrier(jnp.sum(pair * (source[4][:, None, :] - target[4][:, :, None]), axis=2))
                    weights = weights + lax.optimization_barrier(jnp.sum(pair, axis=2))
        return (inflow, weights)
    inflow, weights = lax.map(one_column, jnp.arange(extent_x * extent_y, dtype=jnp.int32))
    array_shape = (extent_x, extent_y, extent_z, bin_dimensions)
    return (inflow.reshape(array_shape), weights.reshape(array_shape))

def wrap_fields(relative_placements, smoothed_particle_measure, temp, heat_diffusion_coefficient):
    fields = jnp.concatenate([relative_placements, smoothed_particle_measure[None], temp[None], heat_diffusion_coefficient[None]], axis=0)
    return jnp.pad(fields, ((0, 0), (1, 1), (1, 1), (1, 1), (0, 0)), mode='wrap')

def reference(relative_placements, mass_per_density, opening_heat_level, bin_fill_counts):
    bin_dimensions = opening_heat_level.shape[-1]
    occupied = (jnp.arange(bin_dimensions, dtype=jnp.int32)[None, None, None, :] < bin_fill_counts[..., None]).astype(jnp.float32)
    smoothed_particle_measure = mass_per_density * occupied
    heat_diffusion_coefficient = opening_heat_level ** 2.5
    periodic_enclosure = opening_heat_level.shape[:3]
    opening_index = opening_heat_level
    reference_heat_rate, row_sums = conduct(wrap_fields(relative_placements, smoothed_particle_measure, opening_index, heat_diffusion_coefficient), periodic_enclosure)
    super_interval_length = step_factor / jnp.max(row_sums * occupied)
    leading_subset = opening_index + 2.0 / 15.0 * super_interval_length * reference_heat_rate
    initial_flow, unused_one = conduct(wrap_fields(relative_placements, smoothed_particle_measure, leading_subset, heat_diffusion_coefficient), periodic_enclosure)
    second = 1.5 * leading_subset - 0.5 * opening_index + 0.6 * super_interval_length * initial_flow - 0.4 * super_interval_length * reference_heat_rate
    flow_second, unused_two = conduct(wrap_fields(relative_placements, smoothed_particle_measure, second, heat_diffusion_coefficient), periodic_enclosure)
    final_temp = 25.0 / 12.0 * second - 5.0 / 6.0 * leading_subset - 0.25 * opening_index + 5.0 / 6.0 * super_interval_length * flow_second - 5.0 / 9.0 * super_interval_length * reference_heat_rate
    return final_temp
```

```python
import functools
import itertools
import jax
import jax.numpy as jnp
from jax import lax
from jax.experimental import pallas as pl
from jax.experimental.pallas import tpu as pltpu
from jax.sharding import PartitionSpec as P

AXES = ("gx", "gy", "gz")
MESH = pl.DeviceIdType.MESH
f32, bf16 = jnp.float32, jnp.bfloat16
DIRS = [d for d in itertools.product((-1, 0, 1), repeat=3) if d != (0, 0, 0)]
COLUMNS = [(ex, ey) for ex in (-1, 0, 1) for ey in (-1, 0, 1)]


def split3(tile):
    hi = tile.astype(bf16).astype(f32)
    rest = tile - hi
    mid = rest.astype(bf16).astype(f32)
    return hi, mid, rest - mid


def kernel(dims, block, f_in, out, f_all, k_all, bt, at, w_all, u1, u2, mx, mx_parts, fsend, frecv, usend, urecv, msend, mrecv):
    bx, by, bz = block
    lanes = f_in.shape[-1]
    me = [lax.axis_index(a) for a in AXES]
    row = lax.broadcasted_iota(jnp.int32, (8, lanes), 0)

    def neighbour(d):
        return tuple(lax.rem(me[k] + (d[k] + dims[k]), dims[k]) if d[k] else me[k] for k in range(3))

    def peer(axis, hop):
        return tuple(lax.rem(me[k] + hop, dims[k]) if k == axis else me[k] for k in range(3))

    barrier = pltpu.get_barrier_semaphore()
    count = 0
    for d in DIRS:
        pl.semaphore_signal(barrier, inc=1, device_id=neighbour(d), device_id_type=MESH)
        count += 1
    for axis in range(3):
        for hop in range(1, dims[axis]):
            pl.semaphore_signal(barrier, inc=1, device_id=peer(axis, hop), device_id_type=MESH)
            count += 1
    pl.semaphore_wait(barrier, count)

    def piece(d, base):
        src, dst = [], []
        for k in range(3):
            n = block[k]
            if d[k] == 0:
                src.append(pl.ds(base, n))
                dst.append(pl.ds(1, n))
            elif d[k] == 1:
                src.append(pl.ds(base + n - 1, 1))
                dst.append(pl.ds(0, 1))
            else:
                src.append(pl.ds(base, 1))
                dst.append(pl.ds(n + 1, 1))
        return tuple(src), tuple(dst)

    def halo_copies(src_ref, base, dst_ref, ssem, rsem):
        copies = []
        for i, d in enumerate(DIRS):
            src, dst = piece(d, base)
            copies.append(
                pltpu.make_async_remote_copy(
                    src_ref=src_ref.at[src],
                    dst_ref=dst_ref.at[dst],
                    send_sem=ssem.at[i],
                    recv_sem=rsem.at[i],
                    device_id=neighbour(d),
                    device_id_type=MESH,
                )
            )
        return copies

    def max_copies(axis):
        start = sum(dims[:axis])
        return [
            pltpu.make_async_remote_copy(
                src_ref=mx.at[axis],
                dst_ref=mx_parts.at[start + hop],
                send_sem=msend.at[start + hop],
                recv_sem=mrecv.at[start + hop],
                device_id=peer(axis, hop),
                device_id_type=MESH,
            )
            for hop in range(1, dims[axis])
        ]

    def start(copies):
        for c in copies:
            c.start()

    def wait(copies):
        for c in copies:
            c.wait()

    def max_result(axis):
        begin = sum(dims[:axis])
        total = mx[axis]
        for hop in range(1, dims[axis]):
            total = jnp.maximum(total, mx_parts[begin + hop])
        return total

    first_halo = halo_copies(f_in, 0, f_all, fsend, frecv)
    start(first_halo)

    def place(col, carry):
        x, y = col // by, col % by
        for z in range(bz):
            f_all[x + 1, y + 1, z + 1] = f_in[x, y, z]
        return carry

    lax.fori_loop(0, bx * by, place, 0)
    wait(first_halo)

    def centred(x, y, z):
        cx = x.astype(f32) - (0.5 * (bx + 1) + 0.5)
        cy = y.astype(f32) - (0.5 * (by + 1) + 0.5)
        cz = z - (0.5 * (bz + 1) + 0.5)
        shift = jnp.where(row == 0, cx, jnp.where(row == 1, cy, cz))
        pos = jnp.where(row < 3, f_all[x, y, z] + shift, 0.0)
        return pos, jnp.sum(pos * pos, axis=0, keepdims=True)

    def sources(col, carry):
        x, y = col // (by + 2), col % (by + 2)
        for z in range(bz + 2):
            pos, norm = centred(x, y, z)
            tile = jnp.where(row < 3, pos, jnp.where(row == 3, norm, jnp.where(row == 4, 1.0, 0.0)))
            hi, mid, lo = split3(tile)
            six = jnp.concatenate([hi, mid, hi, mid, lo, hi], axis=0)
            bt[x, y, z] = six.T.astype(bf16)
        return carry

    lax.fori_loop(0, (bx + 2) * (by + 2), sources, 0)

    def targets(col, carry):
        x, y = col // by, col % by
        for z in range(bz):
            pos, norm = centred(x + 1, y + 1, z + 1)
            tile = jnp.where(row < 3, -2.0 * pos, jnp.where(row == 3, 1.0, jnp.where(row == 4, norm, 0.0)))
            hi, mid, lo = split3(tile)
            at[x, y, z] = jnp.concatenate([hi, hi, mid, mid, hi, lo], axis=0).astype(bf16)
        return carry

    lax.fori_loop(0, bx * by, targets, 0)

    def spread(dist_sq):
        dist_sq = jnp.maximum(dist_sq, 1e-12)
        near = (1.0 - dist_sq * lax.rsqrt(dist_sq)).astype(bf16)
        near = jnp.maximum(near, jnp.zeros((), bf16))
        return near * near * near

    same = lax.broadcasted_iota(jnp.int32, (lanes, lanes), 0) == lax.broadcasted_iota(
        jnp.int32, (lanes, lanes), 1
    )

    def gen(step, carry):
        zp = step % (bz // 2)
        col = step // (bz // 2)
        x, y, z = col // by, col % by, zp * 2
        t = col * bz + z
        both = jnp.concatenate([at[x, y, z], at[x, y, z + 1]], axis=1)
        for c, (ex, ey) in enumerate(COLUMNS):
            for s in range(4):
                lo_t, hi_t = max(s - 2, 0), min(s, 1)
                a = both[:, lo_t * lanes : (hi_t + 1) * lanes]
                d2 = jnp.dot(bt[x + 1 + ex, y + 1 + ey, z + s], a, preferred_element_type=f32)
                for which in range(lo_t, hi_t + 1):
                    part = d2[:, (which - lo_t) * lanes : (which - lo_t + 1) * lanes]
                    if (ex, ey) == (0, 0) and s == which + 1:
                        part = jnp.where(same, 0.0, part)
                    k_all[t + which, c * 3 + s - which] = spread(part)
        return carry

    lax.fori_loop(0, bx * by * (bz // 2), gen, 0)

    def weigh(u_of):
        def body(col, carry):
            x, y = col // (by + 2), col % (by + 2)
            for z in range(bz + 2):
                tile = f_all[x, y, z]
                v, c = tile[3:4], tile[5:6]
                coef = jnp.where(row < 4, jnp.where(row % 2 == 0, v, v * c), 0.0)
                coef = coef * jnp.where(row < 2, u_of(x, y, z), 1.0)
                hi = coef.astype(bf16).astype(f32)
                w_all[x, y, z] = jnp.concatenate([hi, coef - hi], axis=0).astype(bf16)
            return carry

        lax.fori_loop(0, (bx + 2) * (by + 2), body, 0)

    def apply(u_of, emit, init):
        def body(col, carry):
            x, y = col // by, col % by
            for z in range(bz):
                w = jnp.concatenate(
                    [w_all[x + 1 + ex, y + 1 + ey, z + ez] for ex, ey in COLUMNS for ez in range(3)], axis=1
                )
                block_k = k_all[col * bz + z].reshape(27 * lanes, lanes)
                o = jnp.dot(w, block_k, preferred_element_type=f32)
                o = o[0:8] + o[8:16]
                u = u_of(x + 1, y + 1, z + 1)
                c = f_all[x + 1, y + 1, z + 1, 5:6]
                flow = c * (o[0:1] - u * o[2:3]) + (o[1:2] - u * o[3:4])
                carry = emit(carry, x, y, z, flow, c * o[2:3] + o[3:4])
            return carry

        return lax.fori_loop(0, bx * by, body, init)

    def u0_of(x, y, z):
        return f_all[x, y, z, 4:5]

    def u1_of(x, y, z):
        return u1[x, y, z]

    def u2_of(x, y, z):
        return u2[x, y, z]

    def emit0(carry, x, y, z, flow, rows):
        u1[x + 1, y + 1, z + 1] = flow
        return jnp.maximum(carry, rows * f_all[x + 1, y + 1, z + 1, 6:7])

    weigh(u0_of)
    largest = apply(u0_of, emit0, jnp.zeros((1, lanes), f32))
    mx[0] = jnp.broadcast_to(largest, (8, lanes))
    halo1 = halo_copies(u1, 1, u1, usend.at[0], urecv.at[0])
    max0 = max_copies(0)
    start(halo1)
    start(max0)
    wait(halo1)
    wait(max0)
    mx[1] = max_result(0)
    max1 = max_copies(1)
    start(max1)

    def emit1(carry, x, y, z, flow, rows):
        u2[x + 1, y + 1, z + 1] = flow
        return carry

    weigh(u1_of)
    apply(u1_of, emit1, 0)
    halo2 = halo_copies(u2, 1, u2, usend.at[1], urecv.at[1])
    start(halo2)
    wait(max1)
    mx[2] = max_result(1)
    max2 = max_copies(2)
    start(max2)
    wait(halo2)
    wait(max2)
    step = 2.0 / jnp.max(max_result(2)[0:1], axis=1, keepdims=True)

    def emit2(carry, x, y, z, f2, rows):
        u0 = f_all[x + 1, y + 1, z + 1, 4:5]
        f0, f1 = u1[x + 1, y + 1, z + 1], u2[x + 1, y + 1, z + 1]
        first = u0 + 2.0 / 15.0 * step * f0
        l_first = f0 + 2.0 / 15.0 * step * f1
        l_l_first = f1 + 2.0 / 15.0 * step * f2
        second = 1.5 * first - 0.5 * u0 + 0.6 * step * l_first - 0.4 * step * f0
        l_second = 1.5 * l_first - 0.5 * f0 + 0.6 * step * l_l_first - 0.4 * step * f1
        out[x, y, z] = (
            25.0 / 12.0 * second
            - 5.0 / 6.0 * first
            - 0.25 * u0
            + 5.0 / 6.0 * step * l_second
            - 5.0 / 9.0 * step * f0
        )
        return carry

    weigh(u2_of)
    apply(u2_of, emit2, 0)


def local(relative_placements, mass_per_density, opening_heat_level, bin_fill_counts):
    lanes = opening_heat_level.shape[-1]
    block = opening_heat_level.shape[:3]
    dims = tuple(lax.axis_size(a) for a in AXES)
    occupied = (
        jnp.arange(lanes, dtype=jnp.int32)[None, None, None, :] < bin_fill_counts[..., None]
    ).astype(f32)
    heat = opening_heat_level
    rows = [relative_placements[0], relative_placements[1], relative_placements[2]]
    rows += [mass_per_density * occupied, heat, heat * heat * jnp.sqrt(heat), occupied, jnp.zeros_like(heat)]
    fields = jnp.stack(rows, axis=3)
    outer = tuple(n + 2 for n in block)
    cells = block[0] * block[1] * block[2]
    vmem = pl.BlockSpec(memory_space=pltpu.VMEM)
    dma = pltpu.SemaphoreType.DMA
    n_dirs = len(DIRS)
    final = pl.pallas_call(
        functools.partial(kernel, dims, block),
        out_shape=jax.ShapeDtypeStruct(block + (1, lanes), f32),
        in_specs=[vmem],
        out_specs=vmem,
        scratch_shapes=[
            pltpu.VMEM(outer + (8, lanes), f32),
            pltpu.VMEM((cells, 27, lanes, lanes), bf16),
            pltpu.VMEM(outer + (lanes, 48), bf16),
            pltpu.VMEM(block + (48, lanes), bf16),
            pltpu.VMEM(outer + (16, lanes), bf16),
            pltpu.VMEM(outer + (1, lanes), f32),
            pltpu.VMEM(outer + (1, lanes), f32),
            pltpu.VMEM((3, 8, lanes), f32),
            pltpu.VMEM((sum(dims), 8, lanes), f32),
            dma((n_dirs,)),
            dma((n_dirs,)),
            dma((2, n_dirs)),
            dma((2, n_dirs)),
            dma((sum(dims),)),
            dma((sum(dims),)),
        ],
        compiler_params=pltpu.CompilerParams(
            collective_id=0, has_side_effects=True, vmem_limit_bytes=60 * 1024 * 1024
        ),
    )(fields)
    return final.reshape(heat.shape)


def solution(mesh):
    in_specs = (
        P(None, "gx", "gy", "gz", None),
        P("gx", "gy", "gz", None),
        P("gx", "gy", "gz", None),
        P("gx", "gy", "gz"),
    )
    out_specs = P("gx", "gy", "gz", None)
    return jax.shard_map(local, mesh=mesh, in_specs=in_specs, out_specs=out_specs, check_vma=False)
```

```python
import functools
import itertools
import jax
import jax.numpy as jnp
from jax import lax
from jax.experimental import pallas as pl
from jax.experimental.pallas import tpu as pltpu
from jax.sharding import PartitionSpec as P

AXES = ("gx", "gy", "gz")
MESH = pl.DeviceIdType.MESH
f32, bf16 = jnp.float32, jnp.bfloat16
DIRS = [d for d in itertools.product((-1, 0, 1), repeat=3) if d != (0, 0, 0)]
COLUMNS = [(ex, ey) for ex in (-1, 0, 1) for ey in (-1, 0, 1)]


def split3(tile):
    hi = tile.astype(bf16).astype(f32)
    rest = tile - hi
    mid = rest.astype(bf16).astype(f32)
    return hi, mid, rest - mid


def kernel(dims, block, f_in, out, f_all, k_all, bt, at, w_all, u1, u2, mx, mx_parts, fsend, frecv, usend, urecv, msend, mrecv):
    bx, by, bz = block
    lanes = f_in.shape[-1]
    me = [lax.axis_index(a) for a in AXES]
    row = lax.broadcasted_iota(jnp.int32, (8, lanes), 0)

    def neighbour(d):
        return tuple(lax.rem(me[k] + (d[k] + dims[k]), dims[k]) if d[k] else me[k] for k in range(3))

    def peer(axis, hop):
        return tuple(lax.rem(me[k] + hop, dims[k]) if k == axis else me[k] for k in range(3))

    barrier = pltpu.get_barrier_semaphore()
    count = 0
    for d in DIRS:
        pl.semaphore_signal(barrier, inc=1, device_id=neighbour(d), device_id_type=MESH)
        count += 1
    for axis in range(3):
        for hop in range(1, dims[axis]):
            pl.semaphore_signal(barrier, inc=1, device_id=peer(axis, hop), device_id_type=MESH)
            count += 1
    pl.semaphore_wait(barrier, count)

    def piece(d, base):
        src, dst = [], []
        for k in range(3):
            n = block[k]
            if d[k] == 0:
                src.append(pl.ds(base, n))
                dst.append(pl.ds(1, n))
            elif d[k] == 1:
                src.append(pl.ds(base + n - 1, 1))
                dst.append(pl.ds(0, 1))
            else:
                src.append(pl.ds(base, 1))
                dst.append(pl.ds(n + 1, 1))
        return tuple(src), tuple(dst)

    def halo_copies(src_ref, base, dst_ref, ssem, rsem):
        copies = []
        for i, d in enumerate(DIRS):
            src, dst = piece(d, base)
            copies.append(
                pltpu.make_async_remote_copy(
                    src_ref=src_ref.at[src],
                    dst_ref=dst_ref.at[dst],
                    send_sem=ssem.at[i],
                    recv_sem=rsem.at[i],
                    device_id=neighbour(d),
                    device_id_type=MESH,
                )
            )
        return copies

    def max_copies(axis):
        start = sum(dims[:axis])
        return [
            pltpu.make_async_remote_copy(
                src_ref=mx.at[axis],
                dst_ref=mx_parts.at[start + hop],
                send_sem=msend.at[start + hop],
                recv_sem=mrecv.at[start + hop],
                device_id=peer(axis, hop),
                device_id_type=MESH,
            )
            for hop in range(1, dims[axis])
        ]

    def start(copies):
        for c in copies:
            c.start()

    def wait(copies):
        for c in copies:
            c.wait()

    def max_result(axis):
        begin = sum(dims[:axis])
        total = mx[axis]
        for hop in range(1, dims[axis]):
            total = jnp.maximum(total, mx_parts[begin + hop])
        return total

    first_halo = halo_copies(f_in, 0, f_all, fsend, frecv)
    start(first_halo)

    def place(col, carry):
        x, y = col // by, col % by
        for z in range(bz):
            f_all[x + 1, y + 1, z + 1] = f_in[x, y, z]
        return carry

    lax.fori_loop(0, bx * by, place, 0)

    def centred(x, y, z):
        cx = jnp.asarray(x, jnp.int32).astype(f32) - (0.5 * (bx + 1) + 0.5)
        cy = jnp.asarray(y, jnp.int32).astype(f32) - (0.5 * (by + 1) + 0.5)
        cz = z - (0.5 * (bz + 1) + 0.5)
        shift = jnp.where(row == 0, cx, jnp.where(row == 1, cy, cz))
        pos = jnp.where(row < 3, f_all[x, y, z] + shift, 0.0)
        return pos, jnp.sum(pos * pos, axis=0, keepdims=True)

    def source(x, y, z):
        pos, norm = centred(x, y, z)
        tile = jnp.where(row < 3, pos, jnp.where(row == 3, norm, jnp.where(row == 4, 1.0, 0.0)))
        hi, mid, lo = split3(tile)
        six = jnp.concatenate([hi, mid, hi, mid, lo, hi], axis=0)
        bt[x, y, z] = six.T.astype(bf16)

    def own_sources(col, carry):
        for z in range(bz):
            source(col // by + 1, col % by + 1, z + 1)
        return carry

    lax.fori_loop(0, bx * by, own_sources, 0)

    def targets(col, carry):
        x, y = col // by, col % by
        for z in range(bz):
            pos, norm = centred(x + 1, y + 1, z + 1)
            tile = jnp.where(row < 3, -2.0 * pos, jnp.where(row == 3, 1.0, jnp.where(row == 4, norm, 0.0)))
            hi, mid, lo = split3(tile)
            at[x, y, z] = jnp.concatenate([hi, hi, mid, mid, hi, lo], axis=0).astype(bf16)
        return carry

    lax.fori_loop(0, bx * by, targets, 0)

    def spread(dist_sq):
        dist_sq = jnp.maximum(dist_sq, 1e-12)
        near = (1.0 - dist_sq * lax.rsqrt(dist_sq)).astype(bf16)
        near = jnp.maximum(near, jnp.zeros((), bf16))
        return near * near * near

    same = lax.broadcasted_iota(jnp.int32, (lanes, lanes), 0) == lax.broadcasted_iota(
        jnp.int32, (lanes, lanes), 1
    )

    def pairs(x, y, sx, sy, c, own, ends):
        for zp in range(bz // 2):
            z = 2 * zp
            both = jnp.concatenate([at[x, y, z], at[x, y, z + 1]], axis=1)
            for s in range(4):
                rim = (zp == 0 and s == 0) or (zp == bz // 2 - 1 and s == 3)
                if rim != ends:
                    continue
                lo_t, hi_t = max(s - 2, 0), min(s, 1)
                a = both[:, lo_t * lanes : (hi_t + 1) * lanes]
                d2 = jnp.dot(bt[sx, sy, z + s], a, preferred_element_type=f32)
                for which in range(lo_t, hi_t + 1):
                    part = d2[:, (which - lo_t) * lanes : (which - lo_t + 1) * lanes]
                    if own and s == which + 1:
                        part = jnp.where(same, 0.0, part)
                    k_all[(x * by + y) * bz + z + which, c * 3 + s - which] = spread(part)

    for c, (ex, ey) in enumerate(COLUMNS):
        nx, ny = bx - abs(ex), by - abs(ey)
        group = 3 if nx * ny % 3 == 0 else 2 if nx * ny % 2 == 0 else 1

        def inner(step, carry, c=c, ex=ex, ey=ey, ny=ny, group=group):
            for k in range(group):
                i = step * group + k
                x, y = max(0, -ex) + i // ny, max(0, -ey) + i % ny
                pairs(x, y, x + 1 + ex, y + 1 + ey, c, (ex, ey) == (0, 0), False)
            return carry

        lax.fori_loop(0, nx * ny // group, inner, 0)

    wait(first_halo)

    def rim_sources(col, carry):
        for z in range(bz + 2):
            source(col // (by + 2), col % (by + 2), z)
        return carry

    lax.fori_loop(0, (bx + 2) * (by + 2), rim_sources, 0)

    for side in (-1, 1):

        def rim_x(e, carry, side=side):
            x = bx - 1 if side == 1 else 0
            for y in range(by):
                pairs(x, y, x + 1 + side, y + e, (side + 1) * 3 + e, False, False)
            return carry

        def rim_y(e, carry, side=side):
            y = by - 1 if side == 1 else 0
            for x in range(bx):
                pairs(x, y, x + e, y + 1 + side, e * 3 + side + 1, False, False)
            return carry

        lax.fori_loop(0, 3, rim_x, 0)
        lax.fori_loop(0, 3, rim_y, 0)

    def ends(col, carry):
        x, y = col // by, col % by
        for c, (ex, ey) in enumerate(COLUMNS):
            pairs(x, y, x + 1 + ex, y + 1 + ey, c, False, True)
        return carry

    lax.fori_loop(0, bx * by, ends, 0)

    def weigh(u_of):
        def body(col, carry):
            x, y = col // (by + 2), col % (by + 2)
            for z in range(bz + 2):
                tile = f_all[x, y, z]
                v, c = tile[3:4], tile[5:6]
                coef = jnp.where(row < 4, jnp.where(row % 2 == 0, v, v * c), 0.0)
                coef = coef * jnp.where(row < 2, u_of(x, y, z), 1.0)
                hi = coef.astype(bf16).astype(f32)
                w_all[x, y, z] = jnp.concatenate([hi, coef - hi], axis=0).astype(bf16)
            return carry

        lax.fori_loop(0, (bx + 2) * (by + 2), body, 0)

    def apply(u_of, emit, init):
        def body(col, carry):
            x, y = col // by, col % by
            for z in range(bz):
                w = jnp.concatenate(
                    [w_all[x + 1 + ex, y + 1 + ey, z + ez] for ex, ey in COLUMNS for ez in range(3)], axis=1
                )
                block_k = k_all[col * bz + z].reshape(27 * lanes, lanes)
                o = jnp.dot(w, block_k, preferred_element_type=f32)
                o = o[0:8] + o[8:16]
                u = u_of(x + 1, y + 1, z + 1)
                c = f_all[x + 1, y + 1, z + 1, 5:6]
                flow = c * (o[0:1] - u * o[2:3]) + (o[1:2] - u * o[3:4])
                carry = emit(carry, x, y, z, flow, c * o[2:3] + o[3:4])
            return carry

        return lax.fori_loop(0, bx * by, body, init)

    def u0_of(x, y, z):
        return f_all[x, y, z, 4:5]

    def u1_of(x, y, z):
        return u1[x, y, z]

    def u2_of(x, y, z):
        return u2[x, y, z]

    def emit0(carry, x, y, z, flow, rows):
        u1[x + 1, y + 1, z + 1] = flow
        return jnp.maximum(carry, rows * f_all[x + 1, y + 1, z + 1, 6:7])

    weigh(u0_of)
    largest = apply(u0_of, emit0, jnp.zeros((1, lanes), f32))
    mx[0] = jnp.broadcast_to(largest, (8, lanes))
    halo1 = halo_copies(u1, 1, u1, usend.at[0], urecv.at[0])
    max0 = max_copies(0)
    start(halo1)
    start(max0)
    wait(halo1)
    wait(max0)
    mx[1] = max_result(0)
    max1 = max_copies(1)
    start(max1)

    def emit1(carry, x, y, z, flow, rows):
        u2[x + 1, y + 1, z + 1] = flow
        return carry

    weigh(u1_of)
    apply(u1_of, emit1, 0)
    halo2 = halo_copies(u2, 1, u2, usend.at[1], urecv.at[1])
    start(halo2)
    wait(max1)
    mx[2] = max_result(1)
    max2 = max_copies(2)
    start(max2)
    wait(halo2)
    wait(max2)
    step = 2.0 / jnp.max(max_result(2)[0:1], axis=1, keepdims=True)

    def emit2(carry, x, y, z, f2, rows):
        u0 = f_all[x + 1, y + 1, z + 1, 4:5]
        f0, f1 = u1[x + 1, y + 1, z + 1], u2[x + 1, y + 1, z + 1]
        first = u0 + 2.0 / 15.0 * step * f0
        l_first = f0 + 2.0 / 15.0 * step * f1
        l_l_first = f1 + 2.0 / 15.0 * step * f2
        second = 1.5 * first - 0.5 * u0 + 0.6 * step * l_first - 0.4 * step * f0
        l_second = 1.5 * l_first - 0.5 * f0 + 0.6 * step * l_l_first - 0.4 * step * f1
        out[x, y, z] = (
            25.0 / 12.0 * second
            - 5.0 / 6.0 * first
            - 0.25 * u0
            + 5.0 / 6.0 * step * l_second
            - 5.0 / 9.0 * step * f0
        )
        return carry

    weigh(u2_of)
    apply(u2_of, emit2, 0)


def local(relative_placements, mass_per_density, opening_heat_level, bin_fill_counts):
    lanes = opening_heat_level.shape[-1]
    block = opening_heat_level.shape[:3]
    dims = tuple(lax.axis_size(a) for a in AXES)
    occupied = (
        jnp.arange(lanes, dtype=jnp.int32)[None, None, None, :] < bin_fill_counts[..., None]
    ).astype(f32)
    heat = opening_heat_level
    rows = [relative_placements[0], relative_placements[1], relative_placements[2]]
    rows += [mass_per_density * occupied, heat, heat * heat * jnp.sqrt(heat), occupied, jnp.zeros_like(heat)]
    fields = jnp.stack(rows, axis=3)
    outer = tuple(n + 2 for n in block)
    cells = block[0] * block[1] * block[2]
    vmem = pl.BlockSpec(memory_space=pltpu.VMEM)
    dma = pltpu.SemaphoreType.DMA
    n_dirs = len(DIRS)
    final = pl.pallas_call(
        functools.partial(kernel, dims, block),
        out_shape=jax.ShapeDtypeStruct(block + (1, lanes), f32),
        in_specs=[vmem],
        out_specs=vmem,
        scratch_shapes=[
            pltpu.VMEM(outer + (8, lanes), f32),
            pltpu.VMEM((cells, 27, lanes, lanes), bf16),
            pltpu.VMEM(outer + (lanes, 48), bf16),
            pltpu.VMEM(block + (48, lanes), bf16),
            pltpu.VMEM(outer + (16, lanes), bf16),
            pltpu.VMEM(outer + (1, lanes), f32),
            pltpu.VMEM(outer + (1, lanes), f32),
            pltpu.VMEM((3, 8, lanes), f32),
            pltpu.VMEM((sum(dims), 8, lanes), f32),
            dma((n_dirs,)),
            dma((n_dirs,)),
            dma((2, n_dirs)),
            dma((2, n_dirs)),
            dma((sum(dims),)),
            dma((sum(dims),)),
        ],
        compiler_params=pltpu.CompilerParams(
            collective_id=0, has_side_effects=True, vmem_limit_bytes=60 * 1024 * 1024
        ),
    )(fields)
    return final.reshape(heat.shape)


def solution(mesh):
    in_specs = (
        P(None, "gx", "gy", "gz", None),
        P("gx", "gy", "gz", None),
        P("gx", "gy", "gz", None),
        P("gx", "gy", "gz"),
    )
    out_specs = P("gx", "gy", "gz", None)
    return jax.shard_map(local, mesh=mesh, in_specs=in_specs, out_specs=out_specs, check_vma=False)
```
